32 devices in a mesh: left: 8 (over y, x, core), right: 4 (over z).
Axes of the slice: x: 2, y: 2, z: 4, core: 2. Of those that a mesh axis runs over, the one named last changes fastest.
Arguments:
- signal: float32 [256, 256, 1024], P(None, 'left', 'right'), may hold values from -6 to 6
- symbol_x: float32 [256], replicated, may hold values from 0.3 to 3
- symbol_y: float32 [256], replicated, may hold values from 0.3 to 3
- symbol_z: float32 [1024], replicated, may hold values from 0.3 to 3
Outputs:
- spectrum: float32 [128, 128, 512], P('left', 'right')
The draws below stay inside these ranges and needn't reach their ends.
All inputs are finite; a program needn't handle non-finite values.
Results may differ from the reference program's by a relative error of at most 0.000096.
Values sent between devices are 32-bit elements; how exact they have to be, the bound alone decides.
A program may use at most 128 MiB of HBM per device.

```python
import jax
import jax.numpy as jnp
from jax import lax

GRID_X = 256
GRID_Y = 256
GRID_Z = 1024


def steps_of(stream_key, extent, shards, smallest, largest):
    gain = 1.0
    for position, blocks in shards:
        steps = jax.random.uniform(jax.random.fold_in(jax.random.fold_in(stream_key, 6), position), (blocks,), jnp.float32, smallest / len(shards), largest / len(shards))
        gain = gain * jnp.repeat(jnp.exp(steps), extent[position] // blocks).reshape((-1,) + (1,) * (len(extent) - 1 - position))
    return gain


def normal_values(stream_key, extent, spread, most, split=(), dtype=jnp.bfloat16):
    level = steps_of(stream_key, extent, split, -0.22, 0.18) if split else 1.0
    result = jax.random.normal(stream_key, extent, jnp.float32) * spread * level
    return jnp.minimum(jnp.maximum(result, -most), most).astype(dtype)


def setup_inputs(seed: int = 0) -> dict:
    splits = jax.random.split(jax.random.key(seed), 5)
    return {
        "signal": normal_values(splits[0], (GRID_X, GRID_Y, GRID_Z), 1.0, 6.0, ((1, 8), (2, 4)), jnp.float32),
        "symbol_x": jnp.clip(jax.random.uniform(splits[1], (GRID_X,), jnp.float32, 0.3, 3.0), 0.3, 3.0),
        "symbol_y": jnp.clip(jax.random.uniform(splits[2], (GRID_Y,), jnp.float32, 0.3, 3.0), 0.3, 3.0),
        "symbol_z": jnp.clip(jax.random.uniform(splits[3], (GRID_Z,), jnp.float32, 0.3, 3.0), 0.3, 3.0),
    }


def transform_table(count):
    rank = jnp.arange(count)
    angle = (jnp.pi / (4 * count)) * (((2 * rank[:, None] + 1) * (2 * rank[None, :] + 1)) % (8 * count)).astype(jnp.float32)
    return jnp.cos(angle) * (2.0 / count) ** 0.5


def transform_dim(values, dim):
    moved = jnp.tensordot(values, transform_table(values.shape[dim]), axes=([dim], [0]), precision=lax.Precision.HIGHEST)
    return jnp.moveaxis(moved, -1, dim)


def reference(signal, symbol_x, symbol_y, symbol_z):
    spectrum = signal
    spectrum = transform_dim(spectrum, 0)
    spectrum = lax.slice_in_dim(spectrum, 0, GRID_X // 2, axis=0)
    spectrum = transform_dim(spectrum, 1)
    spectrum = lax.slice_in_dim(spectrum, 0, GRID_Y // 2, axis=1)
    spectrum = transform_dim(spectrum, 2)
    spectrum = lax.slice_in_dim(spectrum, 0, GRID_Z // 2, axis=2)
    symbol = symbol_x[:GRID_X // 2][:, None, None] + symbol_y[:GRID_Y // 2][None, :, None] + symbol_z[:GRID_Z // 2][None, None, :]
    spectrum = spectrum * ((1.0 - 0.2 * symbol) / (1.0 + 0.2 * symbol))
    return spectrum
```

```python
import functools

import jax
import jax.numpy as jnp
import numpy as np
from jax import lax
from jax.experimental import pallas as pl
from jax.experimental.pallas import tpu as pltpu
from jax.sharding import PartitionSpec as P

MESH = pl.DeviceIdType.MESH
LANES = 128
ROWS = 8
LAG = 2


def kept_table(count):
    rank = np.arange(count)
    odd = 2 * rank + 1
    angle = np.pi / (4 * count) * ((odd[:, None] * odd[None, : count // 2]) % (8 * count))
    return np.cos(angle) * (2.0 / count) ** 0.5


def two_halves(table):
    high = table.astype(np.float32).astype(jnp.bfloat16)
    rest = table - high.astype(np.float64)
    return np.stack([high, rest.astype(np.float32).astype(jnp.bfloat16)])


def split(values):
    high = values.astype(jnp.bfloat16)
    return high, (values - high.astype(jnp.float32)).astype(jnp.bfloat16)


def product(first, second):
    dot = functools.partial(jnp.dot, preferred_element_type=jnp.float32)
    return dot(first[0], second[0]) + (dot(first[0], second[1]) + dot(first[1], second[0]))


def kernel(
    lefts, rights, chunks,
    signal, table_x, table_y, table_z, symbol_x, symbol_y, symbol_z, out,
    held, tx, ty, tz, first, lines, second, pencils,
    held_sem, table_sem, send1, recv1, send2, recv2,
):
    left, right = lax.axis_index("left"), lax.axis_index("right")
    tiles, blocks, size_x = held.shape[0], held.shape[1], held.shape[2]
    modes_x, own_y = first.shape[1], first.shape[2]
    share_x, size_y = lines.shape[1], lines.shape[2]
    share_y = size_y // 2 // rights
    step = share_x // chunks
    width = blocks * LANES

    def tile_copy(t, b):
        return pltpu.make_async_copy(
            signal.at[:, pl.ds(t * ROWS, ROWS), pl.ds(b * LANES, LANES)],
            held.at[t, b], held_sem.at[t, b])

    copy_x = pltpu.make_async_copy(table_x, tx, table_sem.at[0])
    copy_y = pltpu.make_async_copy(table_y, ty, table_sem.at[1])
    copy_z = pltpu.make_async_copy(table_z, tz, table_sem.at[2])
    copy_x.start()
    for t in range(tiles):
        for b in range(blocks):
            tile_copy(t, b).start()
    copy_y.start()
    copy_z.start()

    barrier = pltpu.get_barrier_semaphore()
    for o in range(1, lefts):
        pl.semaphore_signal(barrier, 1, device_id=(lax.rem(left + o, lefts), right), device_id_type=MESH)
    for o in range(1, rights):
        pl.semaphore_signal(barrier, 1, device_id=(left, lax.rem(right + o, rights)), device_id_type=MESH)

    copy_x.wait()

    def stage1(t, carry):
        for b in range(blocks):
            tile_copy(t, b).wait()
        for y in range(ROWS):
            values = jnp.concatenate(
                [held.at[t, b].reshape(size_x * ROWS, LANES)[pl.ds(y, size_x, stride=ROWS), :] for b in range(blocks)],
                axis=1)
            result = product((tx[0], tx[1]), split(values))
            for b in range(blocks):
                first.at[b].reshape(modes_x * own_y, LANES)[pl.ds(t * ROWS + y, modes_x, stride=own_y), :] = (
                    result[:, b * LANES : (b + 1) * LANES])
        return carry

    lax.fori_loop(0, tiles, stage1, 0)
    pl.semaphore_wait(barrier, lefts + rights - 2)

    def send_left(c, o):
        to = lax.rem(left + o, lefts)
        return pltpu.make_async_remote_copy(
            src_ref=first.at[:, pl.ds(to * share_x + c * step, step)],
            dst_ref=lines.at[:, pl.ds(c * step, step), pl.ds(pl.multiple_of(left * own_y, own_y), own_y), :],
            send_sem=send1.at[o, c], recv_sem=recv1.at[o, c],
            device_id=(to, right), device_id_type=MESH)

    def send_right(c, o):
        to = lax.rem(right + o, rights)
        return pltpu.make_async_remote_copy(
            src_ref=second.at[pl.ds(c * step, step), pl.ds(pl.multiple_of(to * share_y, share_y), share_y), :],
            dst_ref=pencils.at[pl.ds(c * step, step), :, pl.ds(pl.multiple_of(right * width, width), width)],
            send_sem=send2.at[o, c], recv_sem=recv2.at[o, c],
            device_id=(left, to), device_id_type=MESH)

    def start1(c, carry):
        for o in range(1, lefts):
            send_left(c, o).start()
        return carry

    lax.fori_loop(0, chunks, start1, 0)

    def own1(x, carry):
        lines[:, pl.ds(x, 1), pl.ds(pl.multiple_of(left * own_y, own_y), own_y), :] = (
            first[:, pl.ds(left * share_x + x, 1)])
        return carry

    lax.fori_loop(0, share_x, own1, 0)
    copy_y.wait()
    copy_z.wait()

    pick = lax.broadcasted_iota(jnp.int32, (share_y, symbol_y.shape[1]), 1) == (
        right * share_y + lax.broadcasted_iota(jnp.int32, (share_y, symbol_y.shape[1]), 0))
    part_y = jnp.sum(jnp.where(pick, symbol_y[...], 0.0), axis=1, keepdims=True)
    modes_z = out.shape[2]

    def stage23(c, carry):
        @pl.when(c < chunks)
        def _():
            for o in range(1, lefts):
                send_left(c, o).wait_recv()
            for s in range(step):
                x = c * step + s
                values = jnp.concatenate([lines[b, x] for b in range(blocks)], axis=1)
                result = product((ty[0], ty[1]), split(values))
                second[x] = result
            for o in range(1, rights):
                send_right(c, o).start()
            for s in range(step):
                x = c * step + s
                pencils[x, :, pl.ds(pl.multiple_of(right * width, width), width)] = (
                    second[x, pl.ds(pl.multiple_of(right * share_y, share_y), share_y), :])

        @pl.when(c >= LAG)
        def _():
            d = c - LAG
            for o in range(1, rights):
                send_right(d, o).wait_recv()
            values = pencils[pl.ds(d * step, step)].reshape(step * share_y, pencils.shape[2])
            result = product(split(values), (tz[0], tz[1]))
            for s in range(step):
                x = d * step + s
                symbol = (symbol_x[left * share_x + x] + part_y) + symbol_z[:, :modes_z]
                out[x] = result[s * share_y : (s + 1) * share_y] * ((1.0 - 0.2 * symbol) / (1.0 + 0.2 * symbol))
        return carry

    lax.fori_loop(0, chunks + LAG, stage23, 0)

    def finish(c, carry):
        for o in range(1, lefts):
            send_left(c, o).wait_send()
        for o in range(1, rights):
            send_right(c, o).wait_send()
        return carry

    lax.fori_loop(0, chunks, finish, 0)


def body(lefts, rights, signal, symbol_x, symbol_y, symbol_z):
    size_x, own_y, own_z = signal.shape
    size_y, size_z = own_y * lefts, own_z * rights
    modes_x, modes_y, modes_z = size_x // 2, size_y // 2, size_z // 2
    share_x, share_y = modes_x // lefts, modes_y // rights
    chunks = min(8, share_x)
    blocks, tiles = own_z // LANES, own_y // ROWS
    table_x = two_halves(kept_table(size_x).T)
    table_y = two_halves(kept_table(size_y).T)
    table_z = two_halves(kept_table(size_z))
    vmem = pl.BlockSpec(memory_space=pltpu.VMEM)
    any_ = pl.BlockSpec(memory_space=pl.ANY)
    smem = pl.BlockSpec(memory_space=pltpu.SMEM)
    dma = pltpu.SemaphoreType.DMA
    return pl.pallas_call(
        functools.partial(kernel, lefts, rights, chunks),
        out_shape=jax.ShapeDtypeStruct((share_x, share_y, modes_z), jnp.float32),
        in_specs=[any_] * 4 + [smem, vmem, vmem],
        out_specs=vmem,
        scratch_shapes=[
            pltpu.VMEM((tiles, blocks, size_x, ROWS, LANES), jnp.float32),
            pltpu.VMEM(table_x.shape, jnp.bfloat16),
            pltpu.VMEM(table_y.shape, jnp.bfloat16),
            pltpu.VMEM(table_z.shape, jnp.bfloat16),
            pltpu.VMEM((blocks, modes_x, own_y, LANES), jnp.float32),
            pltpu.VMEM((blocks, share_x, size_y, LANES), jnp.float32),
            pltpu.VMEM((share_x, modes_y, own_z), jnp.float32),
            pltpu.VMEM((share_x, share_y, size_z), jnp.float32),
            dma((tiles, blocks)),
            dma((3,)),
            dma((lefts, chunks)),
            dma((lefts, chunks)),
            dma((rights, chunks)),
            dma((rights, chunks)),
        ],
        compiler_params=pltpu.CompilerParams(
            collective_id=0, has_side_effects=True, vmem_limit_bytes=62 * 2**20),
    )(signal, table_x, table_y, table_z, symbol_x, symbol_y[None, :], symbol_z[None, :])


def solution(mesh):
    lefts, rights = mesh.shape["left"], mesh.shape["right"]
    in_specs = (P(None, "left", "right"), P(), P(), P())
    out_specs = P("left", "right", None)
    return jax.shard_map(
        functools.partial(body, lefts, rights), mesh=mesh, in_specs=in_specs, out_specs=out_specs, check_vma=False)
```

```python
import functools

import jax
import jax.numpy as jnp
import numpy as np
from jax import lax
from jax.experimental import pallas as pl
from jax.experimental.pallas import tpu as pltpu
from jax.sharding import PartitionSpec as P

MESH = pl.DeviceIdType.MESH
LANES = 128
ROWS = 8
LAG = 2
AHEAD = 2


def kept_table(count):
    rank = np.arange(count)
    odd = 2 * rank + 1
    angle = np.pi / (4 * count) * ((odd[:, None] * odd[None, : count // 2]) % (8 * count))
    return np.cos(angle) * (2.0 / count) ** 0.5


def two_halves(table):
    high = table.astype(np.float32).astype(jnp.bfloat16)
    rest = table - high.astype(np.float64)
    return np.stack([high, rest.astype(np.float32).astype(jnp.bfloat16)])


def split(values):
    high = values.astype(jnp.bfloat16)
    return high, (values - high.astype(jnp.float32)).astype(jnp.bfloat16)


def product(first, second):
    dot = functools.partial(jnp.dot, preferred_element_type=jnp.float32)
    return dot(first[0], second[0]) + (dot(first[0], second[1]) + dot(first[1], second[0]))


def kernel(
    lefts, rights, chunks,
    signal, table_x, table_y, table_z, symbol_x, symbol_y, symbol_z, out,
    held, tx, ty, tz, first, lines, second, pencils,
    held_sem, table_sem, send0, recv0, send1, recv1, send2, recv2,
):
    left, right = lax.axis_index("left"), lax.axis_index("right")
    tiles, blocks, size_x = held.shape[0], held.shape[1], held.shape[2]
    modes_x, own_y = first.shape[0], first.shape[2]
    share_x, size_y = lines.shape[1], lefts * own_y
    share_y = size_y // 2 // rights
    step = share_x // chunks
    width = blocks * LANES

    def tile_copy(t, b):
        return pltpu.make_async_copy(
            signal.at[:, pl.ds(t * ROWS, ROWS), pl.ds(b * LANES, LANES)],
            held.at[t, b], held_sem.at[t, b])

    copy_x = pltpu.make_async_copy(table_x, tx, table_sem.at[0])
    copy_y = pltpu.make_async_copy(table_y, ty, table_sem.at[1])
    copy_z = pltpu.make_async_copy(table_z, tz, table_sem.at[2])
    copy_x.start()
    for t in range(min(AHEAD, tiles)):
        for b in range(blocks):
            tile_copy(t, b).start()

    barrier = pltpu.get_barrier_semaphore()
    for o in range(1, lefts):
        pl.semaphore_signal(barrier, 1, device_id=(lax.rem(left + o, lefts), right), device_id_type=MESH)
    for o in range(1, rights):
        pl.semaphore_signal(barrier, 1, device_id=(left, lax.rem(right + o, rights)), device_id_type=MESH)

    copy_x.wait()

    def send_tile(t, o):
        to = lax.rem(left + o, lefts)
        return pltpu.make_async_remote_copy(
            src_ref=first.at[pl.ds(to * share_x, step), :, pl.ds(pl.multiple_of(t * ROWS, ROWS), ROWS), :],
            dst_ref=lines.at[left, pl.ds(0, step), :, pl.ds(pl.multiple_of(t * ROWS, ROWS), ROWS), :],
            send_sem=send0.at[o, t], recv_sem=recv0.at[o, t],
            device_id=(to, right), device_id_type=MESH)

    def send_left(c, o):
        to = lax.rem(left + o, lefts)
        return pltpu.make_async_remote_copy(
            src_ref=first.at[pl.ds(to * share_x + c * step, step)],
            dst_ref=lines.at[left, pl.ds(c * step, step)],
            send_sem=send1.at[o, c], recv_sem=recv1.at[o, c],
            device_id=(to, right), device_id_type=MESH)

    def send_right(c, o):
        to = lax.rem(right + o, rights)
        return pltpu.make_async_remote_copy(
            src_ref=second.at[pl.ds(c * step, step), pl.ds(pl.multiple_of(to * share_y, share_y), share_y), :],
            dst_ref=pencils.at[right, pl.ds(c * step, step)],
            send_sem=send2.at[o, c], recv_sem=recv2.at[o, c],
            device_id=(left, to), device_id_type=MESH)

    def stage1(t, carry):
        for b in range(blocks):
            tile_copy(t, b).wait()

        @pl.when(t + AHEAD < tiles)
        def _():
            for b in range(blocks):
                tile_copy(t + AHEAD, b).start()

        for y in range(ROWS):
            values = jnp.concatenate(
                [held.at[t, b].reshape(size_x * ROWS, LANES)[pl.ds(y, size_x, stride=ROWS), :] for b in range(blocks)],
                axis=1)
            result = product((tx[0], tx[1]), split(values))
            for b in range(blocks):
                first.reshape(modes_x * blocks * own_y, LANES)[
                    pl.ds(b * own_y + t * ROWS + y, modes_x, stride=blocks * own_y), :] = (
                    result[:, b * LANES : (b + 1) * LANES])

        @pl.when(t == 0)
        def _():
            pl.semaphore_wait(barrier, lefts + rights - 2)

        for o in range(1, lefts):
            send_tile(t, o).start()
        return carry

    def start1(c, carry):
        for o in range(1, lefts):
            send_left(c, o).start()
        return carry

    lax.fori_loop(0, tiles, stage1, 0)
    lax.fori_loop(1, chunks, start1, 0)
    copy_y.start()
    copy_z.start()

    def own1(x, carry):
        lines[left, x] = first[left * share_x + x]
        return carry

    lax.fori_loop(0, share_x, own1, 0)
    copy_y.wait()
    copy_z.wait()

    pick = lax.broadcasted_iota(jnp.int32, (share_y, symbol_y.shape[1]), 1) == (
        right * share_y + lax.broadcasted_iota(jnp.int32, (share_y, symbol_y.shape[1]), 0))
    part_y = jnp.sum(jnp.where(pick, symbol_y[...], 0.0), axis=1, keepdims=True)
    modes_z = out.shape[2]

    def stage23(c, carry):
        @pl.when(c < chunks)
        def _():
            @pl.when(c == 0)
            def _():
                for t in range(tiles):
                    for o in range(1, lefts):
                        send_tile(t, o).wait_recv()

            @pl.when(c > 0)
            def _():
                for o in range(1, lefts):
                    send_left(c, o).wait_recv()

            for s in range(step):
                x = c * step + s
                values = jnp.concatenate([lines[:, x, b].reshape(size_y, LANES) for b in range(blocks)], axis=1)
                result = product((ty[0], ty[1]), split(values))
                second[x] = result
            for o in range(1, rights):
                send_right(c, o).start()
            for s in range(step):
                x = c * step + s
                pencils[right, x] = second[x, pl.ds(pl.multiple_of(right * share_y, share_y), share_y), :]

        @pl.when(c >= LAG)
        def _():
            d = c - LAG
            for o in range(1, rights):
                send_right(d, o).wait_recv()
            values = jnp.concatenate(
                [pencils[p, pl.ds(d * step, step)].reshape(step * share_y, width) for p in range(rights)], axis=1)
            result = product(split(values), (tz[0], tz[1]))
            for s in range(step):
                x = d * step + s
                symbol = (symbol_x[left * share_x + x] + part_y) + symbol_z[:, :modes_z]
                out[x] = result[s * share_y : (s + 1) * share_y] * ((1.0 - 0.2 * symbol) / (1.0 + 0.2 * symbol))
        return carry

    lax.fori_loop(0, chunks + LAG, stage23, 0)

    def finish(c, carry):
        @pl.when(c > 0)
        def _():
            for o in range(1, lefts):
                send_left(c, o).wait_send()

        for o in range(1, rights):
            send_right(c, o).wait_send()
        return carry

    for t in range(tiles):
        for o in range(1, lefts):
            send_tile(t, o).wait_send()

    lax.fori_loop(0, chunks, finish, 0)


def body(lefts, rights, signal, symbol_x, symbol_y, symbol_z):
    size_x, own_y, own_z = signal.shape
    size_y, size_z = own_y * lefts, own_z * rights
    modes_x, modes_y, modes_z = size_x // 2, size_y // 2, size_z // 2
    share_x, share_y = modes_x // lefts, modes_y // rights
    chunks = min(8, share_x)
    blocks, tiles = own_z // LANES, own_y // ROWS
    table_x = two_halves(kept_table(size_x).T)
    table_y = two_halves(kept_table(size_y).T)
    table_z = two_halves(kept_table(size_z))
    vmem = pl.BlockSpec(memory_space=pltpu.VMEM)
    any_ = pl.BlockSpec(memory_space=pl.ANY)
    smem = pl.BlockSpec(memory_space=pltpu.SMEM)
    dma = pltpu.SemaphoreType.DMA
    return pl.pallas_call(
        functools.partial(kernel, lefts, rights, chunks),
        out_shape=jax.ShapeDtypeStruct((share_x, share_y, modes_z), jnp.float32),
        in_specs=[any_] * 4 + [smem, vmem, vmem],
        out_specs=vmem,
        scratch_shapes=[
            pltpu.VMEM((tiles, blocks, size_x, ROWS, LANES), jnp.float32),
            pltpu.VMEM(table_x.shape, jnp.bfloat16),
            pltpu.VMEM(table_y.shape, jnp.bfloat16),
            pltpu.VMEM(table_z.shape, jnp.bfloat16),
            pltpu.VMEM((modes_x, blocks, own_y, LANES), jnp.float32),
            pltpu.VMEM((lefts, share_x, blocks, own_y, LANES), jnp.float32),
            pltpu.VMEM((share_x, modes_y, own_z), jnp.float32),
            pltpu.VMEM((rights, share_x, share_y, own_z), jnp.float32),
            dma((tiles, blocks)),
            dma((3,)),
            dma((lefts, tiles)),
            dma((lefts, tiles)),
            dma((lefts, chunks)),
            dma((lefts, chunks)),
            dma((rights, chunks)),
            dma((rights, chunks)),
        ],
        compiler_params=pltpu.CompilerParams(
            collective_id=0, has_side_effects=True, vmem_limit_bytes=62 * 2**20),
    )(signal, table_x, table_y, table_z, symbol_x, symbol_y[None, :], symbol_z[None, :])


def solution(mesh):
    lefts, rights = mesh.shape["left"], mesh.shape["right"]
    in_specs = (P(None, "left", "right"), P(), P(), P())
    out_specs = P("left", "right", None)
    return jax.shard_map(
        functools.partial(body, lefts, rights), mesh=mesh, in_specs=in_specs, out_specs=out_specs, check_vma=False)
```
